32 devices in a mesh: seq: 16 (over z, x, core), head: 2 (over y).
Axes of the slice: x: 2, y: 2, z: 4, core: 2. Of those that a mesh axis runs over, the one named last changes fastest.
Arguments:
- tokens: bfloat16 [8192, 1024], P('seq'), may hold values from -6 to 6
- mem_query_w: bfloat16 [1024, 1024], P(None, 'head'), may hold values from -0.1875 to 0.1875
- mem_key_w: bfloat16 [1024, 1024], P(None, 'head'), may hold values from -0.1875 to 0.1875
- mem_value_w: bfloat16 [1024, 1024], P(None, 'head'), may hold values from -0.1875 to 0.1875
- mem_in: float32 [1024, 1024], P(None, 'head'), may hold values from -0.1875 to 0.1875
- mem_out: float32 [1024, 1024], P('head'), may hold values from -0.1875 to 0.1875
- forget_levels: float32 [16, 1024], P(None, 'head'), may hold values from 0.003 to 0.3
- momentum_levels: float32 [16, 1024], P(None, 'head'), may hold values from 0.2 to 0.9
- step_levels: float32 [16, 1024], P(None, 'head'), may hold values from 0.02 to 0.2
- plan: int32 [16], P('seq'), may hold values from 0 to 15
- norm_gain: float32 [1024], replicated, may hold values from 0.5 to 1.5
- attn_query_w: bfloat16 [1024, 1024], P(None, 'head'), may hold values from -1 to 1
- attn_key_w: bfloat16 [1024, 1024], P(None, 'head'), may hold values from -4 to 4
- attn_value_w: bfloat16 [1024, 1024], P(None, 'head'), may hold values from -0.1875 to 0.1875
- attn_out_w: bfloat16 [1024, 1024], P('head'), may hold values from -0.25 to 0.25
Outputs:
- layer_out: bfloat16 [8192, 1024], P('seq', 'head')
The draws below stay inside these ranges and needn't reach their ends.
All inputs are finite; a program needn't handle non-finite values.
Results may differ from the reference program's by a relative error of at most 0.014.
Values may be sent and summed in bfloat16 or wider, within the bound.
No kernel may reach another device: no remote copies, remote signals or barrier semaphores. Data moves between devices by JAX's collectives and lax.ppermute only.
A program may use at most 192 MiB of HBM per device.

```python
import math
import jax
import jax.numpy as jnp
from jax import lax

D = 1024
HEAD_DIM = 64
MEM_HID = 1024
LEVELS = 16
SPAN = 8
TOK_DEV = 512
GROUPS = 16
LENGTH = 8192


def attention_pair(key):
    shared = jax.random.normal(jax.random.fold_in(key, 11), (D, D), jnp.float32) / math.sqrt(D)
    others = jax.random.normal(jax.random.fold_in(key, 12), (D, D), jnp.float32) / math.sqrt(D)
    return (shared, others)


def draw_attn_query_w(key, part):
    shared, others = attention_pair(key)
    return jnp.clip(shared, -1.0, 1.0).astype(jnp.bfloat16)


def draw_attn_key_w(key, part):
    shared, others = attention_pair(key)
    return jnp.clip(others, -4.0, 4.0).astype(jnp.bfloat16)


def touch_ends(array, key, smallest, largest):
    extent = array.shape
    spot = [jax.random.randint(jax.random.fold_in(key, axis), (), 0, extent[axis]) for axis in range(len(extent))]
    array = array.at[tuple(spot)].set(smallest)
    longest = extent.index(max(extent))
    spot[longest] = (spot[longest] + 1) % extent[longest]
    return array.at[tuple(spot)].set(largest)


def spiked(drawn, stream_key, source, target, shards_of, factor):
    def block_of(position):
        return (jnp.arange(drawn.shape[position]) // (drawn.shape[position] // shards_of)).reshape((-1,) + (1,) * (drawn.ndim - 1 - position))

    near = jax.random.permutation(stream_key, shards_of)[block_of(target)]
    far = (block_of(target) + shards_of // 2) % shards_of
    return jnp.where((block_of(source) == near) | (block_of(source) == far), factor * drawn, drawn)


def shard_levels(own_key, extent, split, least, largest):
    factor_of = 1.0
    for position, shards_of in split:
        steps = jax.random.uniform(jax.random.fold_in(jax.random.fold_in(own_key, 6), position), (shards_of,), jnp.float32, least / len(split), largest / len(split))
        factor_of = factor_of * jnp.repeat(jnp.exp(steps), extent[position] // shards_of).reshape((-1,) + (1,) * (len(extent) - 1 - position))
    return factor_of


def scatter_about(rng, extent, spread, most, split=(), kind=jnp.bfloat16):
    factor_of = shard_levels(rng, extent, split, -0.22, 0.18) if split else 1.0
    result = jax.random.normal(rng, extent, jnp.float32) * spread * factor_of
    return jnp.minimum(jnp.maximum(result, -most), most).astype(kind)


def heavy_noise(own_key, dims, width, limit, shards, heavy, kind=jnp.bfloat16):
    result = width * jax.random.normal(own_key, dims, jnp.float32)
    if shards:
        result = result * shard_levels(own_key, dims, shards, -0.22, 0.18)
    return jnp.clip(spiked(result, jax.random.fold_in(own_key, 3), *heavy), -limit, limit).astype(kind)


def setup_inputs(seed: int = 0) -> dict:
    splits = jax.random.split(jax.random.key(seed), 16)
    tokens = scatter_about(splits[0], (LENGTH, D), 1.0, 6.0, ((0, 16),))
    mem_query_w = scatter_about(splits[1], (D, D), D ** -0.5, 0.1875, ((1, 2),))
    mem_key_w = scatter_about(splits[2], (D, D), D ** -0.5, 0.1875, ((1, 2),))
    mem_value_w = scatter_about(splits[3], (D, D), D ** -0.5, 0.1875, ((1, 2),))
    mem_in = scatter_about(splits[4], (D, MEM_HID), D ** -0.5, 0.1875, ((1, 2),), jnp.float32)
    mem_out = scatter_about(splits[5], (MEM_HID, D), MEM_HID ** -0.5, 0.1875, ((0, 2),), jnp.float32)
    forget_levels = jnp.clip(jnp.exp(math.log(0.3) - 4.6051702 * jax.random.uniform(splits[6], (LEVELS, MEM_HID), jnp.float32) ** shard_levels(splits[6], (LEVELS, MEM_HID), ((1, 2),), -0.2, 0.2)), 0.003, 0.3)
    momentum_levels = jnp.clip(0.2 + 0.7 * jax.random.uniform(splits[7], (LEVELS, MEM_HID), jnp.float32) ** shard_levels(splits[7], (LEVELS, MEM_HID), ((1, 2),), -0.2, 0.2), 0.2, 0.9)
    step_levels = jnp.clip(jnp.exp(math.log(0.2) - 2.3025851 * jax.random.uniform(splits[8], (LEVELS, MEM_HID), jnp.float32) ** shard_levels(splits[8], (LEVELS, MEM_HID), ((1, 2),), -0.2, 0.2)), 0.02, 0.2)
    plan = touch_ends(jax.random.randint(splits[9], (GROUPS,), 0, LEVELS), jax.random.fold_in(splits[9], 1), 0, LEVELS - 1).astype(jnp.int32)
    norm_gain = jnp.clip(1.0 + 0.1 * jax.random.normal(splits[10], (D,), jnp.float32), 0.5, 1.5)
    attn_query_w = draw_attn_query_w(jax.random.fold_in(splits[15], 71), 0)
    attn_key_w = draw_attn_key_w(jax.random.fold_in(splits[15], 71), 0)
    attn_value_w = scatter_about(splits[13], (D, D), D ** -0.5, 0.1875, ((1, 2),))
    attn_out_w = heavy_noise(splits[14], (D, D), D ** -0.5, 0.25, ((0, 2),), (0, 1, 2, 2.0))
    return {"tokens": tokens, "mem_query_w": mem_query_w, "mem_key_w": mem_key_w, "mem_value_w": mem_value_w, "mem_in": mem_in, "mem_out": mem_out, "forget_levels": forget_levels, "momentum_levels": momentum_levels, "step_levels": step_levels, "plan": plan, "norm_gain": norm_gain, "attn_query_w": attn_query_w, "attn_key_w": attn_key_w, "attn_value_w": attn_value_w, "attn_out_w": attn_out_w}


highest = lax.Precision.HIGHEST
epsilon = 1e-06

def silu_slope(values):
    sigmoid = jax.nn.sigmoid(values)
    return sigmoid * (1.0 + values * (1.0 - sigmoid))

def project(left, weight):
    return jnp.dot(left, weight, preferred_element_type=jnp.float32).astype(jnp.bfloat16)

def normalize(retrieved, norm_gain):
    mean_square = lax.optimization_barrier(jnp.mean(retrieved * retrieved, axis=-1, keepdims=True))
    return (retrieved * lax.rsqrt(mean_square + epsilon) * norm_gain).astype(jnp.bfloat16)

def window_attend(query, keys, values, block_index, head_dim):
    query_count = query.shape[0]
    key_count = keys.shape[0]
    head_count = query.shape[1] // head_dim
    query_heads = query.reshape(query_count, head_count, head_dim).astype(jnp.float32)
    key_heads = keys.reshape(key_count, head_count, head_dim).astype(jnp.float32)
    value_heads = values.reshape(key_count, head_count, head_dim).astype(jnp.float32)
    scores = jnp.einsum('qhd,khd->hqk', query_heads, key_heads) * head_dim ** (-0.5)
    span_rows = key_count - query_count
    distance = span_rows + jnp.arange(query_count, dtype=jnp.int32)[:, None] - jnp.arange(key_count, dtype=jnp.int32)[None, :]
    key_pos = (block_index * query_count - span_rows + jnp.arange(key_count, dtype=jnp.int32))[None, :]
    allowed = (distance >= 0) & (distance < span_rows) & (key_pos >= 0)
    scores = jnp.where(allowed[None], scores, -1e+30)
    row_peak = lax.optimization_barrier(jnp.max(scores, axis=-1, keepdims=True))
    weights = jnp.exp(scores - row_peak)
    probabilities = (weights / lax.optimization_barrier(jnp.sum(weights, axis=-1, keepdims=True))).astype(jnp.bfloat16)
    context = jnp.einsum('hqk,khd->qhd', probabilities.astype(jnp.float32), value_heads)
    return context.reshape(query_count, head_count * head_dim).astype(jnp.bfloat16)

def reference(tokens, mem_query_w, mem_key_w, mem_value_w, mem_in, mem_out, forget_levels, momentum_levels, step_levels, plan, norm_gain, attn_query_w, attn_key_w, attn_value_w, attn_out_w):
    mem_query = project(tokens, mem_query_w).reshape(GROUPS, TOK_DEV, D)
    mem_key = project(tokens, mem_key_w).reshape(GROUPS, TOK_DEV, D)
    mem_value = project(tokens, mem_value_w).reshape(GROUPS, TOK_DEV, D)

    def group_step(state_now, inputs):
        speed_in, speed_out, weight_in, weight_out = state_now
        query_rows, key_rows, value_rows, chosen = inputs
        keys_wide = key_rows.astype(jnp.float32)
        pre_act = jnp.dot(keys_wide, mem_in, precision=highest)
        hidden = jax.nn.silu(pre_act)
        predicted = jnp.dot(hidden, mem_out, precision=highest)
        residual_err = 2.0 / TOK_DEV * (predicted - value_rows.astype(jnp.float32))
        grad_out = jnp.dot(hidden.T, residual_err, precision=highest)
        slope_term = jnp.dot(residual_err, mem_out.T, precision=highest) * silu_slope(pre_act)
        grad_in = jnp.dot(keys_wide.T, slope_term, precision=highest)
        query_wide = query_rows.astype(jnp.float32)
        retrieved = jnp.dot(jax.nn.silu(jnp.dot(query_wide, weight_in, precision=highest)), weight_out, precision=highest)
        forget = forget_levels[chosen]
        momentum = momentum_levels[chosen]
        step_rate = step_levels[chosen]
        speed_in = momentum[None, :] * speed_in - step_rate[None, :] * grad_in
        speed_out = momentum[:, None] * speed_out - step_rate[:, None] * grad_out
        weight_in = (1.0 - forget)[None, :] * weight_in + speed_in
        weight_out = (1.0 - forget)[:, None] * weight_out + speed_out
        return ((speed_in, speed_out, weight_in, weight_out), retrieved)
    initial = (jnp.zeros_like(mem_in), jnp.zeros_like(mem_out), mem_in, mem_out)
    last_state, retrieved = lax.scan(group_step, initial, (mem_query, mem_key, mem_value, plan))
    normed = normalize(retrieved.reshape(LENGTH, D), norm_gain)
    att_query = project(normed, attn_query_w)
    att_key = project(normed, attn_key_w)
    att_value = project(normed, attn_value_w)
    span_rows = SPAN * TOK_DEV
    padding = jnp.zeros((span_rows, D), jnp.bfloat16)
    key_padded = jnp.concatenate([padding, att_key], axis=0)
    value_padded = jnp.concatenate([padding, att_value], axis=0)

    def attend_block(block_index):
        begin = block_index * TOK_DEV
        query_block = lax.dynamic_slice_in_dim(att_query, begin, TOK_DEV, 0)
        key_block = lax.dynamic_slice_in_dim(key_padded, begin, span_rows + TOK_DEV, 0)
        value_block = lax.dynamic_slice_in_dim(value_padded, begin, span_rows + TOK_DEV, 0)
        return window_attend(query_block, key_block, value_block, block_index, HEAD_DIM)
    context = lax.map(attend_block, jnp.arange(GROUPS, dtype=jnp.int32)).reshape(LENGTH, D)
    return project(context, attn_out_w)
```

```python
import functools
import math

import jax
import jax.numpy as jnp
from jax import lax
from jax.experimental import pallas as pl
from jax.experimental.pallas import tpu as pltpu
from jax.sharding import PartitionSpec as P

HEAD_DIM = 64
SPAN = 8
LANES = 128
PLANE = SPAN // 2
LOWEST = -1e30

epsilon = 1e-06
bf16 = jnp.bfloat16
f32 = jnp.float32


def dot(left, right, left_dim=1, right_dim=0):
    return lax.dot_general(
        left, right, (((left_dim,), (right_dim,)), ((), ())), preferred_element_type=f32
    )


def head_parts(value, axis):
    count = lax.axis_size("head")
    size = value.shape[axis] // count
    place = lax.axis_index("head")
    return [
        lax.dynamic_slice_in_dim(value, (place + k) % count * size, size, axis)
        for k in range(count)
    ]


def from_heads(mine):
    count = lax.axis_size("head")
    return [mine] + [
        lax.ppermute(mine, "head", [(j, (j - k) % count) for j in range(count)])
        for k in range(1, count)
    ]


def sum_over_heads(pieces):
    count = lax.axis_size("head")
    total = pieces[0]
    for k in range(1, count):
        total = total + lax.ppermute(
            pieces[k].astype(bf16), "head", [(j, (j + k) % count) for j in range(count)]
        ).astype(f32)
    return total


def seq_shift(value, by):
    length = lax.axis_size("seq")
    return lax.ppermute(value, "seq", [(i, i + by) for i in range(length - by)])


def seq_swap(value, bit):
    length = lax.axis_size("seq")
    return lax.ppermute(value, "seq", [(i, i ^ bit) for i in range(length)])


def scan_kernel(momentum, keep, rate, start, change, entering):
    speed = jnp.zeros_like(start)
    weight = start[...]
    for group in range(change.shape[0]):
        row = pl.ds(group, 1)
        entering[group] = weight.astype(bf16)
        speed = momentum[row, :] * speed - rate[row, :] * change[group].astype(f32)
        weight = keep[row, :] * weight + speed


def entering_weights(momentum, keep, rate, start, change):
    groups, rows, cols = change.shape
    block = rows // 4 if rows % 64 == 0 else rows
    gates = pl.BlockSpec((groups, cols), lambda i: (0, 0))
    part = pl.BlockSpec((groups, block, cols), lambda i: (0, i, 0))
    return pl.pallas_call(
        scan_kernel,
        grid=(rows // block,),
        in_specs=[gates, gates, gates, pl.BlockSpec((block, cols), lambda i: (i, 0)), part],
        out_specs=part,
        out_shape=jax.ShapeDtypeStruct(change.shape, bf16),
        name="entering_scan",
    )(momentum, keep, rate, start, change)


def attend_kernel(blocks_here, first, last, span, meta, query, *refs):
    kv = refs[: 2 * blocks_here]
    refs = refs[2 * blocks_here :]
    if not first:
        acc_in, peak_in, total_in = refs[:3]
        refs = refs[3:]
    if last:
        out = refs[0]
        acc, peak, total = refs[1:]
    else:
        acc, peak, total = refs
    rows, lanes = query.shape
    count = kv[0].shape[0]
    if first:
        acc[...] = jnp.zeros_like(acc)
        total[...] = jnp.zeros_like(total)
        peak[...] = jnp.full(peak.shape, LOWEST, f32)
    else:
        acc[...] = acc_in[...]
        total[...] = total_in[...]
        peak[...] = peak_in[...]
    tile = min(256, rows)
    left = lax.broadcasted_iota(jnp.int32, (tile, lanes), 1) < HEAD_DIM

    def step(number, masked):
        keys, values = kv[2 * number], kv[2 * number + 1]
        offset = (meta[0] - meta[1 + number]) * count
        for low in range(0, rows, tile):
            piece = pl.ds(low, tile)
            old_peak = peak[piece, :]
            outs, peaks, scales, sums = [], [], [], []
            if masked:
                distance = (
                    offset
                    + low
                    + lax.broadcasted_iota(jnp.int32, (tile, count), 0)
                    - lax.broadcasted_iota(jnp.int32, (tile, count), 1)
                )
                allowed = (distance >= 0) & (distance < span * count)
            for side in range(2):
                mine = left if side == 0 else jnp.logical_not(left)
                q = jnp.where(mine, query[piece, :], jnp.zeros((), bf16))
                scores = dot(q, keys[...], 1, 1)
                if masked:
                    scores = jnp.where(allowed, scores, LOWEST)
                before = old_peak[:, side * HEAD_DIM : side * HEAD_DIM + 1]
                now = jnp.maximum(before, jnp.max(scores, axis=1, keepdims=True))
                weights = jnp.exp2(scores - now)
                sums.append(jnp.sum(weights, axis=1, keepdims=True))
                peaks.append(now)
                scales.append(jnp.exp2(before - now))
                outs.append(dot(weights.astype(bf16), values[...]))
            pick = lambda pair: jnp.where(left, pair[0], pair[1])
            scale = pick(scales)
            acc[piece, :] = acc[piece, :] * scale + pick(outs)
            total[piece, :] = total[piece, :] * scale + pick(sums)
            peak[piece, :] = pick(peaks)

    for number in range(blocks_here):
        gap = meta[0] - meta[1 + number]
        seen = (meta[1 + number] >= 0) & (gap >= 0) & (gap <= span)
        edge = (gap == 0) | (gap == span)

        @pl.when(seen & edge)
        def _():
            step(number, True)

        @pl.when(seen & jnp.logical_not(edge))
        def _():
            step(number, False)

    if last:
        out[...] = (acc[...] / total[...]).astype(bf16)


def attend(meta, query, blocks, carry, last):
    rows, cols = query.shape
    pairs = cols // LANES
    lane_block = pl.BlockSpec((rows, LANES), lambda i, meta: (0, i))
    kv_specs, kv_args = [], []
    for block in blocks:
        count = block.shape[0]
        kv_specs.append(pl.BlockSpec((count, LANES), lambda i, meta: (0, i)))
        kv_specs.append(pl.BlockSpec((count, LANES), lambda i, meta: (0, i + pairs)))
        kv_args += [block, block]
    state = jax.ShapeDtypeStruct((rows, cols), f32)
    first = carry is None
    scratch = [pltpu.VMEM((rows, LANES), f32)] * 3 if last else []
    keys = sum(block.shape[0] for block in blocks)
    return pl.pallas_call(
        functools.partial(attend_kernel, len(blocks), first, last, SPAN),
        grid_spec=pltpu.PrefetchScalarGridSpec(
            num_scalar_prefetch=1,
            grid=(pairs,),
            in_specs=[lane_block] + kv_specs + ([] if first else [lane_block] * 3),
            out_specs=lane_block if last else [lane_block] * 3,
            scratch_shapes=scratch,
        ),
        out_shape=jax.ShapeDtypeStruct((rows, cols), bf16) if last else [state] * 3,
        cost_estimate=pl.CostEstimate(
            flops=4 * rows * keys * cols * 4,
            bytes_accessed=8 * rows * cols,
            transcendentals=rows * keys * cols // HEAD_DIM,
        ),
        name="attend",
    )(meta, query, *kv_args, *([] if first else carry))


def shards(
    tokens,
    mem_query_w,
    mem_key_w,
    mem_value_w,
    mem_in,
    mem_out,
    forget_levels,
    momentum_levels,
    step_levels,
    plan,
    norm_gain,
    attn_query_w,
    attn_key_w,
    attn_value_w,
    attn_out_w,
):
    tok_rows, width = tokens.shape
    units = mem_in.shape[1]
    heads = lax.axis_size("head")
    groups = lax.axis_size("seq")
    place = lax.axis_index("seq")

    key_parts = from_heads(dot(tokens, mem_key_w).astype(bf16))
    query_parts = from_heads(dot(tokens, mem_query_w).astype(bf16))
    value_mine = dot(tokens, mem_value_w)
    in_parts = [part.astype(bf16) for part in head_parts(mem_in, 0)]
    out_parts = [part.astype(bf16) for part in head_parts(mem_out, 1)]

    pre_act = sum(dot(k, w) for k, w in zip(key_parts, in_parts))
    sigmoid = jax.nn.sigmoid(pre_act)
    hidden = (pre_act * sigmoid).astype(bf16)
    slope = sigmoid * (1.0 + pre_act * (1.0 - sigmoid))
    predicted = [dot(hidden, w) for w in out_parts]
    predicted[0] = predicted[0] - value_mine.astype(bf16).astype(f32)
    error_parts = from_heads((2.0 / tok_rows * sum_over_heads(predicted)).astype(bf16))
    grad_out = [dot(e, hidden, 0, 0) for e in error_parts]
    slope_term = (sum(dot(e, w, 1, 1) for e, w in zip(error_parts, out_parts)) * slope).astype(bf16)
    grad_in = [dot(k, slope_term, 0, 0) for k in key_parts]

    share = width // groups
    change = jnp.concatenate(
        [
            jnp.concatenate([g.astype(bf16) for g in grads], axis=0).reshape(groups, share, units)
            for grads in (grad_in, grad_out)
        ],
        axis=1,
    )
    change = lax.all_to_all(change, "seq", 0, 0, tiled=True)
    chosen = lax.all_gather(plan, "seq", tiled=True)
    matches = chosen[:, None] == jnp.arange(forget_levels.shape[0], dtype=jnp.int32)[None, :]
    pick = lambda table: jnp.sum(jnp.where(matches[:, :, None], table[None], 0.0), axis=1)
    my_row = (lax.axis_index("head") * (width // heads) + place * share) % width
    start = jnp.concatenate(
        [
            lax.dynamic_slice_in_dim(
                jnp.concatenate(head_parts(mem_in, 0), axis=0), place * share, share, 0
            ),
            lax.dynamic_slice_in_dim(mem_out, my_row, share, 1).T,
        ],
        axis=0,
    )
    entering = entering_weights(
        pick(momentum_levels), 1.0 - pick(forget_levels), pick(step_levels), start, change
    )
    entering = lax.all_to_all(entering, "seq", 0, 0, tiled=True)
    weight_in = entering[:, :share].reshape(width, units)
    weight_out = entering[:, share:].reshape(width, units)

    query_hidden = jax.nn.silu(dot(jnp.concatenate(query_parts, axis=1), weight_in)).astype(bf16)
    own = width // heads
    retrieved = sum_over_heads(
        [dot(query_hidden, weight_out[k * own : (k + 1) * own], 1, 1) for k in range(heads)]
    )
    parts = [part.astype(f32) for part in from_heads(retrieved.astype(bf16))]
    mean_square = sum(jnp.sum(p * p, axis=1, keepdims=True) for p in parts) / width
    inverse = lax.rsqrt(mean_square + epsilon)
    gains = head_parts(norm_gain, 0)
    normed = jnp.concatenate(
        [(p * inverse * g[None, :]).astype(bf16) for p, g in zip(parts, gains)], axis=1
    )

    def turned(weight):
        return jnp.concatenate(head_parts(weight, 0), axis=0)

    cols = attn_query_w.shape[1]
    chunk = cols // 2 if cols % (2 * LANES) == 0 else cols
    chunks = range(0, cols, chunk)
    scale = HEAD_DIM ** (-0.5) * math.log2(math.e)
    att_query = (dot(normed, turned(attn_query_w)) * scale).astype(bf16)
    key_w, value_w = turned(attn_key_w), turned(attn_value_w)
    own_kv = [
        dot(
            normed, jnp.concatenate([key_w[:, c : c + chunk], value_w[:, c : c + chunk]], axis=1)
        ).astype(bf16)
        for c in chunks
    ]
    is_left = place // 2 % 2 == 0
    block = place.astype(jnp.int32)
    contexts = []
    for number, low in enumerate(chunks):
        query = att_query[:, low : low + chunk]
        here = own_kv[number]
        below = seq_shift(here, PLANE)
        across = seq_swap(below, 2)
        further = seq_shift(below, PLANE)
        final = seq_swap(jnp.where(is_left, here, further), 2)
        stages = [
            (here, block, block ^ 1),
            (below, block - PLANE, (block ^ 1) - PLANE),
            (across, (block ^ 2) - PLANE, (block ^ 3) - PLANE),
            (further, block - 2 * PLANE, (block ^ 1) - 2 * PLANE),
            (
                final,
                (block ^ 2) - jnp.where(is_left, 2 * PLANE, 0),
                (block ^ 3) - jnp.where(is_left, 2 * PLANE, 0),
            ),
        ]
        carry = None
        for index, (kv, near, far) in enumerate(stages):
            meta = jnp.stack([block, near, far])
            carry = attend(meta, query, [kv, seq_swap(kv, 1)], carry, index == len(stages) - 1)
        contexts.append(carry)
    out_rows = [attn_out_w[low : low + chunk] for low in chunks]
    out = sum_over_heads(
        [
            sum(dot(c, w) for c, w in zip(contexts, pieces))
            for pieces in zip(*[head_parts(rows, 1) for rows in out_rows])
        ]
    )
    return out.astype(bf16)


def solution(mesh):
    in_specs = (
        P("seq", None),
        P(None, "head"),
        P(None, "head"),
        P(None, "head"),
        P(None, "head"),
        P("head", None),
        P(None, "head"),
        P(None, "head"),
        P(None, "head"),
        P("seq"),
        P(),
        P(None, "head"),
        P(None, "head"),
        P(None, "head"),
        P("head", None),
    )
    out_specs = P("seq", "head")
    return jax.shard_map(shards, mesh=mesh, in_specs=in_specs, out_specs=out_specs, check_vma=False)
```
